32 devices in a mesh: section: 4 (over y, x), tensor: 8 (over z, core).
Axes of the slice: x: 2, y: 2, z: 4, core: 2. Of those that a mesh axis runs over, the one named last changes fastest.
Arguments:
- tokens: bfloat16 [2, 32, 4096], P(None, 'tensor'), may hold values from -24 to 24
- expert_ids: int32 [4, 2, 32, 2], P('section', None, 'tensor'), may hold values from 0 to 7, as said below
- router_weight: bfloat16 [4, 4096, 8], P('section'), may hold values from -0.09375 to 0.09375
- norm_gain: float32 [4, 4096], P('section'), may hold values from 0.1 to 1.9
- gate_weight: bfloat16 [4, 28672, 4096], P('section', 'tensor'), may hold values from -0.09375 to 0.09375
- up_weight: bfloat16 [4, 28672, 4096], P('section', 'tensor'), may hold values from -0.09375 to 0.09375
- down_weight: bfloat16 [4, 28672, 4096], P('section', 'tensor'), may hold values from -0.046875 to 0.046875
Outputs:
- section_outputs: bfloat16 [4, 2, 32, 4096], P('section', None, 'tensor')
The draws below stay inside these ranges and needn't reach their ends.
Inputs may be any that keep to these rules, and one draw needn't show every extreme that they name: `expert_ids`: each token names two different experts. Along the token dimension, in aligned blocks of 4 tokens of one micro-batch and one layer, at most 2 tokens name expert 0 and at most 2 name expert 1; in some micro-batch of every layer every block has exactly 2 of each.
All inputs are finite; a program needn't handle non-finite values.
Results may differ from the reference program's by a relative error of at most 0.0055.
Values may be sent and summed in bfloat16 or wider, within the bound.
No kernel may reach another device: no remote copies, remote signals or barrier semaphores. Data moves between devices by JAX's collectives and lax.ppermute only.
A program may use at most 128 MiB of HBM per device.

```python
import math
import jax
import jax.numpy as jnp
from jax import lax

D = 4096
FF = 14336
EXPERTS = 8
MICRO = 2
TOK_DEV = 4
SLOT = 2
TOK = 32
N_SECTION = 4
N_TENSOR = 8


def draw_tokens(key, part):
    keys = jax.random.split(jax.random.fold_in(key, 11), 3)
    shape = (MICRO, TOK, D)
    row_scale = jnp.exp(jax.random.uniform(keys[0], (MICRO, TOK, 1), jnp.float32, math.log(0.5), math.log(2.0)))
    column_scale = jnp.exp(jax.random.uniform(keys[1], (1, 1, D), jnp.float32, math.log(0.4), math.log(4.0)))
    values = jax.random.normal(keys[2], shape, jnp.float32) * row_scale * column_scale
    return jnp.clip(values, -24.0, 24.0).astype(jnp.bfloat16)


def draw_expert_ids(key, part):
    keys = jax.random.split(jax.random.fold_in(key, 23), 8)
    shape = (N_SECTION, MICRO, N_TENSOR, TOK_DEV)
    full_micro = jax.random.randint(keys[0], (N_SECTION,), 0, MICRO)
    micro_index = jnp.arange(MICRO, dtype=jnp.int32)
    is_full = micro_index[None, :, None] == full_micro[:, None, None]
    counts_zero = jnp.where(is_full, SLOT, jax.random.randint(keys[1], (N_SECTION, MICRO, N_TENSOR), 0, SLOT + 1))
    counts_one = jnp.where(is_full, SLOT, jax.random.randint(keys[2], (N_SECTION, MICRO, N_TENSOR), 0, SLOT + 1))
    position = jnp.arange(TOK_DEV, dtype=jnp.int32)
    scores_zero = jax.random.randint(keys[3], shape, 0, 1 << 20) * TOK_DEV + position
    scores_one = jax.random.randint(keys[4], shape, 0, 1 << 20) * TOK_DEV + position
    rank_zero = jnp.argsort(jnp.argsort(scores_zero, axis=-1), axis=-1).astype(jnp.int32)
    rank_one = jnp.argsort(jnp.argsort(scores_one, axis=-1), axis=-1).astype(jnp.int32)
    names_zero = rank_zero < counts_zero[..., None]
    names_one = rank_one < counts_one[..., None]
    first_alt = 2 + jax.random.randint(keys[5], shape, 0, EXPERTS - 2)
    second_alt = 2 + (first_alt - 2 + 1 + jax.random.randint(keys[6], shape, 0, EXPERTS - 3)) % (EXPERTS - 2)
    first_id = jnp.where(names_zero, 0, jnp.where(names_one, 1, first_alt))
    second_id = jnp.where(names_zero, jnp.where(names_one, 1, first_alt), jnp.where(names_one, first_alt, second_alt))
    swapped = jax.random.randint(keys[7], shape, 0, 2) == 1
    routes = jnp.stack([jnp.where(swapped, second_id, first_id), jnp.where(swapped, first_id, second_id)], axis=-1)
    return routes.reshape(N_SECTION, MICRO, TOK, 2).astype(jnp.int32)


def block_scale(key, shape, cuts, least, high):
    def one(dim, shards_of):
        steps = jax.random.uniform(jax.random.fold_in(jax.random.fold_in(key, 6), dim), (shards_of,), jnp.float32, least / len(cuts), high / len(cuts))
        return jnp.repeat(jnp.exp(steps), shape[dim] // shards_of).reshape((-1,) + (1,) * (len(shape) - dim - 1))

    level = one(*cuts[0])
    for cut in cuts[1:]:
        level = level * one(*cut)
    return level


def normal_values(own_key, extent, spread, most, cuts=(), kind=jnp.bfloat16):
    entries = jax.random.normal(own_key, extent, jnp.float32) * spread
    if len(cuts) > 0:
        entries = block_scale(own_key, extent, cuts, -0.22, 0.18) * entries
    return jnp.clip(entries, min=-most, max=most).astype(kind)


def setup_inputs(seed: int = 0) -> dict:
    arg_keys = jax.random.split(jax.random.key(seed), 8)
    tokens = draw_tokens(jax.random.fold_in(arg_keys[7], 71), 0)
    expert_ids = draw_expert_ids(jax.random.fold_in(arg_keys[7], 71), 0)
    router_weight = normal_values(arg_keys[2], (N_SECTION, D, EXPERTS), D ** -0.5, 0.09375, ((0, 4),))
    norm_gain = jnp.clip(1.0 + 0.18 * jax.random.normal(arg_keys[3], (N_SECTION, D), jnp.float32), 0.1, 1.9)
    gate_weight = normal_values(arg_keys[4], (N_SECTION, 2 * FF, D), D ** -0.5, 0.09375, ((0, 4), (1, 8)))
    up_weight = normal_values(arg_keys[5], (N_SECTION, 2 * FF, D), D ** -0.5, 0.09375, ((0, 4), (1, 8)))
    down_weight = normal_values(arg_keys[6], (N_SECTION, 2 * FF, D), FF ** -0.5, 0.046875, ((0, 4), (1, 8)))
    return {"tokens": tokens, "expert_ids": expert_ids, "router_weight": router_weight, "norm_gain": norm_gain, "gate_weight": gate_weight, "up_weight": up_weight, "down_weight": down_weight}


EPSILON = 1e-05

def normalize(hidden_rows, gain):
    wide = hidden_rows.astype(jnp.float32)
    scale = lax.rsqrt(lax.optimization_barrier(jnp.mean(wide * wide, axis=-1, keepdims=True)) + EPSILON)
    return (wide * scale * gain).astype(jnp.bfloat16)

def mixing_weight(logits, routes, expert):
    routed = (routes[:, 0] == expert) | (routes[:, 1] == expert)
    partner = jnp.where(routes[:, 0] == expert, routes[:, 1], routes[:, 0])
    columns = jnp.arange(logits.shape[1], dtype=jnp.int32)
    partner_logit = lax.optimization_barrier(jnp.sum(jnp.where(columns[None, :] == partner[:, None], logits, 0.0), axis=1))
    value = 1.0 / (1.0 + jnp.exp(partner_logit - logits[:, expert]))
    return (jnp.where(routed, value, 0.0), routed.astype(jnp.int32))

def pickers(flags, slot_count):
    place = jnp.cumsum(flags, axis=1) - 1
    slots = jnp.arange(slot_count, dtype=jnp.int32)
    chosen = (place[:, None, :] == slots[None, :, None]) & (flags[:, None, :] == 1)
    return chosen.astype(jnp.float32)

def project_rows(rows, weight_rows):
    return lax.dot_general(rows, weight_rows, (((1,), (1,)), ((), ())), preferred_element_type=jnp.float32)

def one_layer(hidden_rows, routes, router, gain, w_gate, w_up, w_down):
    normed = normalize(hidden_rows, gain)
    logits = jnp.dot(normed, router, preferred_element_type=jnp.float32)
    blocks = normed.reshape(N_TENSOR, TOK_DEV, D).astype(jnp.float32)
    total = hidden_rows.astype(jnp.float32)
    for expert in range(2):
        weight, flags = mixing_weight(logits, routes, expert)
        picker = pickers(flags.reshape(N_TENSOR, TOK_DEV), SLOT)
        packed = jnp.einsum('bsj,bjd->bsd', picker, blocks, precision=lax.Precision.HIGHEST)
        packed = packed.astype(jnp.bfloat16).reshape(N_TENSOR * SLOT, D)
        gate = project_rows(packed, w_gate[expert * FF:(expert + 1) * FF])
        upward = project_rows(packed, w_up[expert * FF:(expert + 1) * FF])
        hidden = (jax.nn.silu(gate) * upward).astype(jnp.bfloat16)
        slot_out = jnp.dot(hidden, w_down[expert * FF:(expert + 1) * FF], preferred_element_type=jnp.float32)
        output = jnp.einsum('bsj,bsd->bjd', picker, slot_out.reshape(N_TENSOR, SLOT, D), precision=lax.Precision.HIGHEST)
        total = total + weight[:, None] * output.reshape(TOK, D)
    return total.astype(jnp.bfloat16)

def reference(tokens, expert_ids, router_weight, norm_gain, gate_weight, up_weight, down_weight):
    current = tokens
    collected = []
    for layer in range(N_SECTION):

        def run_micro(pair, layer=layer):
            return one_layer(pair[0], pair[1], router_weight[layer], norm_gain[layer], gate_weight[layer], up_weight[layer], down_weight[layer])
        current = lax.map(run_micro, (current, expert_ids[layer]))
        collected.append(current)
    return jnp.stack(collected)
```

```python
import functools

import jax
import jax.numpy as jnp
from jax import lax
from jax.experimental import pallas as pl
from jax.experimental.pallas import tpu as pltpu
from jax.sharding import PartitionSpec as P

EPSILON = 1e-05


def normalize(wide, gain):
    scale = lax.rsqrt(jnp.mean(wide * wide, axis=-1, keepdims=True) + EPSILON)
    return (wide * scale * gain).astype(jnp.bfloat16)


def same_block(shape, count):
    rows = lax.broadcasted_iota(jnp.int32, shape, 0)
    columns = lax.broadcasted_iota(jnp.int32, shape, 1)
    return rows, columns, rows // count == columns // count


def pick_rows(ids_across, ids_down, expert, count, slot_count):
    tokens = ids_across.shape[1]
    slots = tokens // count * slot_count
    flag_across = (ids_across[0:1] == expert) | (ids_across[1:2] == expert)
    flag_down = (ids_down[:, 0:1] == expert) | (ids_down[:, 1:2] == expert)
    rows, columns, same = same_block((tokens, tokens), count)
    earlier = same & (rows < columns) & flag_down
    place = jnp.sum(earlier.astype(jnp.int32), axis=0, keepdims=True)
    slot = lax.broadcasted_iota(jnp.int32, (slots, tokens), 0)
    token = lax.broadcasted_iota(jnp.int32, (slots, tokens), 1)
    return flag_across & (slot // slot_count == token // count) & (slot % slot_count == place)


def place_rows(ids_across, ids_down, expert, count, slot_count):
    tokens = ids_across.shape[1]
    slots = tokens // count * slot_count
    flag_across = (ids_across[0:1] == expert) | (ids_across[1:2] == expert)
    flag_down = (ids_down[:, 0:1] == expert) | (ids_down[:, 1:2] == expert)
    rows, columns, same = same_block((tokens, tokens), count)
    earlier = same & (columns < rows) & flag_across
    place = jnp.sum(earlier.astype(jnp.int32), axis=1, keepdims=True)
    token = lax.broadcasted_iota(jnp.int32, (tokens, slots), 0)
    slot = lax.broadcasted_iota(jnp.int32, (tokens, slots), 1)
    return flag_down & (slot // slot_count == token // count) & (slot % slot_count == place)


def mixing_weight(logits, ids_down, expert):
    routed = (ids_down[:, 0:1] == expert) | (ids_down[:, 1:2] == expert)
    partner = jnp.where(ids_down[:, 0:1] == expert, ids_down[:, 1:2], ids_down[:, 0:1])
    columns = lax.broadcasted_iota(jnp.int32, logits.shape, 1)
    other = jnp.sum(jnp.where(columns == partner, logits, 0.0), axis=1, keepdims=True)
    value = 1.0 / (1.0 + jnp.exp(other - logits[:, expert : expert + 1]))
    return jnp.where(routed, value, 0.0)


def pack_kernel(count, slot_count, hidden_ref, gain_ref, across_ref, down_ref, pack_ref):
    normed = normalize(hidden_ref[...].astype(jnp.float32), gain_ref[...])
    half = pack_ref.shape[0] // 2
    for expert in range(2):
        pick = pick_rows(across_ref[...], down_ref[...], expert, count, slot_count)
        rows = jnp.dot(pick.astype(jnp.bfloat16), normed, preferred_element_type=jnp.float32)
        rows = rows.astype(jnp.bfloat16)
        for device in range(half):
            pack_ref[expert * half + device] = rows


def expert_kernel(
    steps, count, slot_count,
    active_ref, x_ref, hidden_ref, gain_ref, router_ref, across_ref, down_ref,
    gate_ref, up_ref, out_ref_w, part_ref, spread_ref, sum_ref,
):
    step = pl.program_id(0)

    @pl.when((step == 0) & (active_ref[0] == 1))
    def _():
        normed = normalize(hidden_ref[...].astype(jnp.float32), gain_ref[...])
        logits = lax.dot_general(
            normed, router_ref[...], (((1,), (1,)), ((), ())), preferred_element_type=jnp.float32
        )
        ids_across = across_ref[...]
        ids_down = down_ref[...]
        for expert in range(2):
            weight = mixing_weight(logits, ids_down, expert)
            place = place_rows(ids_across, ids_down, expert, count, slot_count)
            spread_ref[expert] = jnp.where(place, weight, 0.0)

    @pl.when(active_ref[0] == 1)
    def _():
        x = x_ref[...].reshape(sum_ref.shape)
        contract = (((1,), (1,)), ((), ()))
        gate = lax.dot_general(x, gate_ref[...], contract, preferred_element_type=jnp.float32)
        upward = lax.dot_general(x, up_ref[...], contract, preferred_element_type=jnp.float32)
        hidden = (jax.nn.silu(gate) * upward).astype(jnp.bfloat16)
        product = jnp.dot(hidden, out_ref_w[...], preferred_element_type=jnp.float32)

        @pl.when(step == 0)
        def _():
            sum_ref[...] = product

        @pl.when(step > 0)
        def _():
            sum_ref[...] += product

    @pl.when((step == steps - 1) & (active_ref[0] == 1))
    def _():
        part_ref[...] = sum_ref[...].reshape(part_ref.shape).astype(jnp.bfloat16)


def run_experts(active, x, hidden, gain, router, across, down, w_gate, w_up, w_down, count, slot_count):
    devices, slots, width = x.shape
    units = w_gate.shape[0]
    tile = max(c for c in (256, 128, 64, 32, 16) if units % c == 0)
    steps = units // tile
    tokens = hidden.shape[0]
    moving = lambda i, a: (i * a[0], 0)
    full = lambda array: pl.BlockSpec(array.shape, lambda i, a: (0,) * array.ndim)
    return pl.pallas_call(
        functools.partial(expert_kernel, steps, count, slot_count),
        grid_spec=pltpu.PrefetchScalarGridSpec(
            num_scalar_prefetch=1,
            grid=(steps,),
            in_specs=[full(x), full(hidden), full(gain), full(router), full(across), full(down)]
            + [pl.BlockSpec((tile, width), moving)] * 3,
            out_specs=[
                pl.BlockSpec(x.shape, lambda i, a: (0, 0, 0)),
                pl.BlockSpec((2, tokens, slots), lambda i, a: (0, 0, 0)),
            ],
            scratch_shapes=[pltpu.VMEM((devices * slots, width), jnp.float32)],
        ),
        out_shape=[
            jax.ShapeDtypeStruct(x.shape, jnp.bfloat16),
            jax.ShapeDtypeStruct((2, tokens, slots), jnp.float32),
        ],
        compiler_params=pltpu.CompilerParams(vmem_limit_bytes=40 * 1024 * 1024),
    )(active, x, hidden, gain, router, across, down, w_gate, w_up, w_down)


def combine_kernel(devices, parts_ref, spread_ref, hidden_ref, result_ref):
    total = hidden_ref[...].astype(jnp.float32)
    slots = spread_ref.shape[2]
    half = devices // 2
    for expert in range(2):
        summed = parts_ref[expert * half].astype(jnp.float32)
        for device in range(1, half):
            summed = summed + parts_ref[expert * half + device].astype(jnp.float32)
        spread = spread_ref[expert]
        for slot in range(slots):
            total = total + spread[:, slot : slot + 1] * summed[slot : slot + 1]
    result_ref[...] = total.astype(jnp.bfloat16)


def body(tokens, expert_ids, router_weight, norm_gain, gate_weight, up_weight, down_weight):
    sections = lax.axis_size("section")
    devices = lax.axis_size("tensor")
    section = lax.axis_index("section")
    micro, count, width = tokens.shape
    slot_count = count // 2
    slots = micro * slot_count
    rows = micro * count
    router = jnp.swapaxes(router_weight[0], 0, 1)
    ids_down = expert_ids[0].reshape(rows, 2)
    ids_across = jnp.swapaxes(ids_down, 0, 1)

    def exchange(blocks):
        return lax.all_to_all(blocks, "tensor", 0, 0, tiled=True)

    pack = pl.pallas_call(
        functools.partial(pack_kernel, count, slot_count),
        out_shape=jax.ShapeDtypeStruct((devices, slots, width), jnp.bfloat16),
    )
    combine = pl.pallas_call(
        functools.partial(combine_kernel, devices),
        out_shape=jax.ShapeDtypeStruct((rows, width), jnp.bfloat16),
    )
    hidden = tokens.reshape(rows, width)
    output = hidden
    for layer in range(sections):
        if layer > 0:
            hidden = lax.ppermute(output, "section", [(layer - 1, layer)])
        x = exchange(pack(hidden, norm_gain, ids_across, ids_down))
        active = (section == layer).astype(jnp.int32).reshape(1)
        partial, spread = run_experts(
            active, x, hidden, norm_gain, router, ids_across, ids_down,
            gate_weight[0], up_weight[0], down_weight[0], count, slot_count,
        )
        result = combine(exchange(partial), spread, hidden)
        output = result if layer == 0 else jnp.where(section == layer, result, output)
    return output.reshape(1, micro, count, width)


def solution(mesh):
    return jax.shard_map(
        body,
        mesh=mesh,
        in_specs=(
            P(None, "tensor", None),
            P("section", None, "tensor", None),
            P("section", None, None),
            P("section", None),
            P("section", "tensor", None),
            P("section", "tensor", None),
            P("section", "tensor", None),
        ),
        out_specs=P("section", None, "tensor", None),
        check_vma=False,
    )
```

```python
import functools

import jax
import jax.numpy as jnp
from jax import lax
from jax.experimental import pallas as pl
from jax.experimental.pallas import tpu as pltpu
from jax.sharding import PartitionSpec as P

EPSILON = 1e-05


def normalize(wide, gain):
    scale = lax.rsqrt(jnp.mean(wide * wide, axis=-1, keepdims=True) + EPSILON)
    return (wide * scale * gain).astype(jnp.bfloat16)


def same_block(shape, count):
    rows = lax.broadcasted_iota(jnp.int32, shape, 0)
    columns = lax.broadcasted_iota(jnp.int32, shape, 1)
    return rows, columns, rows // count == columns // count


def pick_rows(ids_across, ids_down, expert, count, slot_count):
    tokens = ids_across.shape[1]
    slots = tokens // count * slot_count
    flag_across = (ids_across[0:1] == expert) | (ids_across[1:2] == expert)
    flag_down = (ids_down[:, 0:1] == expert) | (ids_down[:, 1:2] == expert)
    rows, columns, same = same_block((tokens, tokens), count)
    earlier = same & (rows < columns) & flag_down
    place = jnp.sum(earlier.astype(jnp.int32), axis=0, keepdims=True)
    slot = lax.broadcasted_iota(jnp.int32, (slots, tokens), 0)
    token = lax.broadcasted_iota(jnp.int32, (slots, tokens), 1)
    return flag_across & (slot // slot_count == token // count) & (slot % slot_count == place)


def place_rows(ids_across, ids_down, expert, count, slot_count):
    tokens = ids_across.shape[1]
    slots = tokens // count * slot_count
    flag_across = (ids_across[0:1] == expert) | (ids_across[1:2] == expert)
    flag_down = (ids_down[:, 0:1] == expert) | (ids_down[:, 1:2] == expert)
    rows, columns, same = same_block((tokens, tokens), count)
    earlier = same & (columns < rows) & flag_across
    place = jnp.sum(earlier.astype(jnp.int32), axis=1, keepdims=True)
    token = lax.broadcasted_iota(jnp.int32, (tokens, slots), 0)
    slot = lax.broadcasted_iota(jnp.int32, (tokens, slots), 1)
    return flag_down & (slot // slot_count == token // count) & (slot % slot_count == place)


def mixing_weight(logits, ids_down, expert):
    routed = (ids_down[:, 0:1] == expert) | (ids_down[:, 1:2] == expert)
    partner = jnp.where(ids_down[:, 0:1] == expert, ids_down[:, 1:2], ids_down[:, 0:1])
    columns = lax.broadcasted_iota(jnp.int32, logits.shape, 1)
    other = jnp.sum(jnp.where(columns == partner, logits, 0.0), axis=1, keepdims=True)
    value = 1.0 / (1.0 + jnp.exp(other - logits[:, expert : expert + 1]))
    return jnp.where(routed, value, 0.0)


def pack_kernel(count, slot_count, hidden_ref, gain_ref, across_ref, down_ref, pack_ref):
    normed = normalize(hidden_ref[...].astype(jnp.float32), gain_ref[...])
    half = pack_ref.shape[0] // 2
    for expert in range(2):
        pick = pick_rows(across_ref[...], down_ref[...], expert, count, slot_count)
        rows = jnp.dot(pick.astype(jnp.bfloat16), normed, preferred_element_type=jnp.float32)
        rows = rows.astype(jnp.bfloat16)
        for device in range(half):
            pack_ref[expert * half + device] = rows


def expert_kernel(
    steps, count, slot_count,
    active_ref, x_ref, hidden_ref, gain_ref, router_ref, across_ref, down_ref,
    gate_ref, up_ref, out_ref_w, part_ref, spread_ref, sum_ref,
):
    step = pl.program_id(0)

    @pl.when((step == 0) & (active_ref[0] == 1))
    def _():
        normed = normalize(hidden_ref[...].astype(jnp.float32), gain_ref[...])
        logits = lax.dot_general(
            normed, router_ref[...], (((1,), (1,)), ((), ())), preferred_element_type=jnp.float32
        )
        ids_across = across_ref[...]
        ids_down = down_ref[...]
        for expert in range(2):
            weight = mixing_weight(logits, ids_down, expert)
            place = place_rows(ids_across, ids_down, expert, count, slot_count)
            spread_ref[expert] = jnp.where(place, weight, 0.0)

    @pl.when(active_ref[0] == 1)
    def _():
        x = x_ref[...].reshape(sum_ref.shape)
        contract = (((1,), (1,)), ((), ()))
        gate = lax.dot_general(x, gate_ref[...], contract, preferred_element_type=jnp.float32)
        upward = lax.dot_general(x, up_ref[...], contract, preferred_element_type=jnp.float32)
        hidden = (jax.nn.silu(gate) * upward).astype(jnp.bfloat16)
        product = jnp.dot(hidden, out_ref_w[...], preferred_element_type=jnp.float32)

        @pl.when(step == 0)
        def _():
            sum_ref[...] = product

        @pl.when(step > 0)
        def _():
            sum_ref[...] += product

    @pl.when((step == steps - 1) & (active_ref[0] == 1))
    def _():
        part_ref[...] = sum_ref[...].reshape(part_ref.shape).astype(jnp.bfloat16)


def run_experts(active, x, hidden, gain, router, across, down, w_gate, w_up, w_down, count, slot_count):
    devices, slots, width = x.shape
    units = w_gate.shape[0]
    tile = max(c for c in (512, 256, 128, 64, 32, 16) if units % c == 0)
    steps = units // tile
    tokens = hidden.shape[0]
    moving = lambda i, a: (i * a[0], 0)
    full = lambda array: pl.BlockSpec(array.shape, lambda i, a: (0,) * array.ndim)
    return pl.pallas_call(
        functools.partial(expert_kernel, steps, count, slot_count),
        grid_spec=pltpu.PrefetchScalarGridSpec(
            num_scalar_prefetch=1,
            grid=(steps,),
            in_specs=[full(x), full(hidden), full(gain), full(router), full(across), full(down)]
            + [pl.BlockSpec((tile, width), moving)] * 3,
            out_specs=[
                pl.BlockSpec(x.shape, lambda i, a: (0, 0, 0)),
                pl.BlockSpec((2, tokens, slots), lambda i, a: (0, 0, 0)),
            ],
            scratch_shapes=[pltpu.VMEM((devices * slots, width), jnp.float32)],
        ),
        out_shape=[
            jax.ShapeDtypeStruct(x.shape, jnp.bfloat16),
            jax.ShapeDtypeStruct((2, tokens, slots), jnp.float32),
        ],
        compiler_params=pltpu.CompilerParams(vmem_limit_bytes=40 * 1024 * 1024),
    )(active, x, hidden, gain, router, across, down, w_gate, w_up, w_down)


def combine_kernel(devices, parts_ref, spread_ref, hidden_ref, result_ref):
    total = hidden_ref[...].astype(jnp.float32)
    slots = spread_ref.shape[2]
    half = devices // 2
    for expert in range(2):
        summed = parts_ref[expert * half].astype(jnp.float32)
        for device in range(1, half):
            summed = summed + parts_ref[expert * half + device].astype(jnp.float32)
        spread = spread_ref[expert]
        for slot in range(slots):
            total = total + spread[:, slot : slot + 1] * summed[slot : slot + 1]
    result_ref[...] = total.astype(jnp.bfloat16)


def body(tokens, expert_ids, router_weight, norm_gain, gate_weight, up_weight, down_weight):
    sections = lax.axis_size("section")
    devices = lax.axis_size("tensor")
    section = lax.axis_index("section")
    micro, count, width = tokens.shape
    slot_count = count // 2
    slots = micro * slot_count
    rows = micro * count
    router = jnp.swapaxes(router_weight[0], 0, 1)
    ids_down = expert_ids[0].reshape(rows, 2)
    ids_across = jnp.swapaxes(ids_down, 0, 1)

    def exchange(blocks):
        return lax.all_to_all(blocks, "tensor", 0, 0, tiled=True)

    pack = pl.pallas_call(
        functools.partial(pack_kernel, count, slot_count),
        out_shape=jax.ShapeDtypeStruct((devices, slots, width), jnp.bfloat16),
    )
    combine = pl.pallas_call(
        functools.partial(combine_kernel, devices),
        out_shape=jax.ShapeDtypeStruct((rows, width), jnp.bfloat16),
    )
    hidden = tokens.reshape(rows, width)
    output = hidden
    for layer in range(sections):
        if layer > 0:
            hidden = lax.ppermute(output, "section", [(layer - 1, layer)])
        x = exchange(pack(hidden, norm_gain, ids_across, ids_down))
        active = (section == layer).astype(jnp.int32).reshape(1)
        partial, spread = run_experts(
            active, x, hidden, norm_gain, router, ids_across, ids_down,
            gate_weight[0], up_weight[0], down_weight[0], count, slot_count,
        )
        result = combine(exchange(partial), spread, hidden)
        output = result if layer == 0 else jnp.where(section == layer, result, output)
    return output.reshape(1, micro, count, width)


def solution(mesh):
    return jax.shard_map(
        body,
        mesh=mesh,
        in_specs=(
            P(None, "tensor", None),
            P("section", None, "tensor", None),
            P("section", None, None),
            P("section", None),
            P("section", "tensor", None),
            P("section", "tensor", None),
            P("section", "tensor", None),
        ),
        out_specs=P("section", None, "tensor", None),
        check_vma=False,
    )
```
